32 devices in a mesh: gx: 4 (over y, x), gy: 8 (over z, core).
Axes of the slice: x: 2, y: 2, z: 4, core: 2. Of those that a mesh axis runs over, the one named last changes fastest.
Arguments:
- q_nodes: bfloat16 [32, 512, 4096], P(('gx', 'gy')), may hold values from -30 to 30, as said below
- k_cache: bfloat16 [32, 1024, 512], P(('gx', 'gy')), may hold values from -6 to 6, as said below
- v_cache: bfloat16 [32, 1024, 512], P(('gx', 'gy')), may hold values from -6 to 6
- k_tree: bfloat16 [32, 512, 512], P(('gx', 'gy')), may hold values from -6 to 6
- v_tree: bfloat16 [32, 512, 512], P(('gx', 'gy')), may hold values from -6 to 6
- anc_bits: int32 [32, 512, 16], P(('gx', 'gy')), may hold values from -2147483648 to 2147483647, as said below
- node_count: int32 [32], P(('gx', 'gy')), may hold values from 1 to 512, as said below
- cache_len: int32 [32], P(('gx', 'gy')), may hold values from 256 to 1024, as said below
- sinks: float32 [64], replicated, may hold values from 5 to 10
- o_weight: bfloat16 [4096, 2880], P(('gx', 'gy')), may hold values from -0.09375 to 0.09375
Outputs:
- attended: bfloat16 [32, 512, 4096], P(('gx', 'gy'))
- projected: bfloat16 [32, 512, 2880], P(('gx', 'gy'))
The draws below stay inside these ranges and needn't reach their ends.
Inputs may be any that keep to these rules, and one draw needn't show every extreme that they name: `q_nodes`: custom draw of queries. `k_cache`: custom draw of keys. `anc_bits`: bit j mod 32 of word j // 32 in row i is set exactly when tree node j is node i or one of its ancestors; node 0 is the root and a node's ancestors have lower indices. `node_count`: write request r as a * 8 + b with b < 8. Where a + b is even, the tree has more than (2) * 128 nodes; elsewhere it has at most 128. Request 0 has 512 nodes. `cache_len`: request 0 has 1024 cached positions.
All inputs are finite; a program needn't handle non-finite values.
Results may differ from the reference program's by a relative error of at most 0.0055.
Values may be sent and summed in bfloat16 or wider, within the bound.
No kernel may reach another device: no remote copies, remote signals or barrier semaphores. Data moves between devices by JAX's collectives and lax.ppermute only.
A program may use at most 192 MiB of HBM per device.

```python
import jax
import jax.numpy as jnp
from jax import lax

QH = 64
KVH = 8
HD = 64
D = 2880
TREE_MAX = 512
BLK = 128
CACHE_MAX = 1024
REQUESTS = 32
N_GY = 8


def tree_tables(key):
    base_key = jax.random.fold_in(key, 11)
    block_count = TREE_MAX // BLK
    request_ids = jnp.arange(REQUESTS, dtype=jnp.int32)
    parity = (request_ids // N_GY + request_ids % N_GY) % 2
    busy_blocks = jax.random.randint(jax.random.fold_in(base_key, 1), (REQUESTS,), block_count - 1, block_count + 1)
    live_blocks = jnp.where(parity == 0, busy_blocks, 1).astype(jnp.int32)
    extra_nodes = jax.random.randint(jax.random.fold_in(base_key, 2), (REQUESTS,), 1, BLK + 1)
    node_total = ((live_blocks - 1) * BLK + extra_nodes).astype(jnp.int32)
    node_total = node_total.at[0].set(TREE_MAX)
    steps_back = jax.random.randint(jax.random.fold_in(base_key, 3), (REQUESTS, TREE_MAX), 1, 5)
    parents = jnp.maximum(jnp.arange(TREE_MAX, dtype=jnp.int32)[None, :] - steps_back, 0).astype(jnp.int32)
    word_count = TREE_MAX // 32
    word_ids = jnp.arange(word_count, dtype=jnp.int32)
    row_ids = jnp.arange(REQUESTS, dtype=jnp.int32)

    def add_node(node_index, bit_table):
        parent_row = bit_table[row_ids, parents[:, node_index]]
        parent_row = jnp.where(node_index > 0, parent_row, jnp.zeros_like(parent_row))
        own_bit = jnp.where(word_ids == node_index // 32, jnp.left_shift(jnp.asarray(1, jnp.int32), node_index % 32), 0).astype(jnp.int32)
        new_row = jnp.bitwise_or(parent_row, own_bit[None, :])
        return lax.dynamic_update_slice(bit_table, new_row[:, None, :], (0, node_index, 0))
    bit_table = lax.fori_loop(0, TREE_MAX, add_node, jnp.zeros((REQUESTS, TREE_MAX, word_count), jnp.int32))
    return (node_total, bit_table)


def draw_node_count(key, part):
    return tree_tables(key)[0]


def draw_anc_bits(key, part):
    return tree_tables(key)[1]


def draw_cache_len(key, part):
    counts = jax.random.randint(jax.random.fold_in(key, 41), (REQUESTS,), CACHE_MAX // 4, CACHE_MAX + 1)
    return counts.astype(jnp.int32).at[0].set(CACHE_MAX)


def draw_k_cache(key, part):
    full_shape = (REQUESTS, CACHE_MAX, KVH * HD)
    values = jnp.clip(jax.random.normal(jax.random.fold_in(key, 21), full_shape, jnp.float32), -6.0, 6.0)
    return values.astype(jnp.bfloat16)


def draw_q_nodes(key, part):
    full_shape = (REQUESTS, TREE_MAX, QH * HD)
    values = jnp.clip(2.0 * jax.random.normal(jax.random.fold_in(key, 31), full_shape, jnp.float32), -12.0, 12.0)
    return values.astype(jnp.bfloat16)


def steps_of(rng, dims, split, smallest, largest):
    gain, own = 1.0, jax.random.fold_in(rng, 6)
    for position, blocks in split:
        steps = jnp.exp(jax.random.uniform(jax.random.fold_in(own, position), (blocks,), jnp.float32, smallest / len(split), largest / len(split)))
        gain = gain * jnp.repeat(steps, dims[position] // blocks).reshape([-1 if axis == position else 1 for axis in range(len(dims))])
    return gain


def bell_draw(key, extent, spread, most, cuts=(), kind=jnp.bfloat16):
    drawn = spread * jax.random.normal(key, extent, jnp.float32)
    if cuts:
        drawn = drawn * steps_of(key, extent, cuts, -0.22, 0.18)
    return jnp.clip(drawn, -most, most).astype(kind)


def setup_inputs(seed: int = 0) -> dict:
    keys = jax.random.split(jax.random.key(seed), 11)
    q_nodes = draw_q_nodes(jax.random.fold_in(keys[10], 71), 0)
    k_cache = draw_k_cache(jax.random.fold_in(keys[10], 71), 0)
    v_cache = bell_draw(keys[2], (REQUESTS, CACHE_MAX, KVH * HD), 1.0, 6.0, ((0, 32),))
    k_tree = bell_draw(keys[3], (REQUESTS, TREE_MAX, KVH * HD), 1.0, 6.0, ((0, 32),))
    v_tree = bell_draw(keys[4], (REQUESTS, TREE_MAX, KVH * HD), 1.0, 6.0, ((0, 32),))
    anc_bits = draw_anc_bits(jax.random.fold_in(keys[10], 71), 0)
    node_count = draw_node_count(jax.random.fold_in(keys[10], 71), 0)
    cache_len = draw_cache_len(jax.random.fold_in(keys[10], 71), 0)
    sinks = jnp.clip(jax.random.uniform(keys[8], (QH,), jnp.float32, 5.0, 10.0), 5.0, 10.0)
    o_weight = bell_draw(keys[9], (QH * HD, D), (QH * HD) ** -0.5, 0.09375, ((0, 32),))
    return dict(q_nodes=q_nodes, k_cache=k_cache, v_cache=v_cache, k_tree=k_tree, v_tree=v_tree, anc_bits=anc_bits, node_count=node_count, cache_len=cache_len, sinks=sinks, o_weight=o_weight)


MASKED = -1.0e30


def unpack_bits(bit_words):
    shift_ids = jnp.arange(32, dtype=jnp.int32)
    bit_flags = jnp.bitwise_and(jnp.right_shift(bit_words[:, :, None], shift_ids), 1)
    return bit_flags.reshape(bit_words.shape[0], bit_words.shape[1] * 32) > 0


def attend_rows(q_rows, tree_ok, cache_keys, cache_values, tree_keys, tree_values, cache_count, sinks):
    row_total = q_rows.shape[0]
    groups = QH // KVH
    head_width = groups * HD
    scale_factor = HD ** -0.5
    cache_ok = jnp.arange(cache_keys.shape[0], dtype=jnp.int32) < cache_count
    tree_mask = jnp.repeat(tree_ok, groups, axis=0)

    def per_kv_head(kv_head):
        q_part = lax.dynamic_slice_in_dim(q_rows, kv_head * head_width, head_width, 1).reshape(row_total * groups, HD)
        key_cache = lax.dynamic_slice_in_dim(cache_keys, kv_head * HD, HD, 1)
        value_cache = lax.dynamic_slice_in_dim(cache_values, kv_head * HD, HD, 1)
        key_tree = lax.dynamic_slice_in_dim(tree_keys, kv_head * HD, HD, 1)
        value_tree = lax.dynamic_slice_in_dim(tree_values, kv_head * HD, HD, 1)
        score_cache = jnp.dot(q_part, key_cache.T, preferred_element_type=jnp.float32) * scale_factor
        score_cache = jnp.where(cache_ok[None, :], score_cache, MASKED)
        score_tree = jnp.dot(q_part, key_tree.T, preferred_element_type=jnp.float32) * scale_factor
        score_tree = jnp.where(tree_mask, score_tree, MASKED)
        sink_rows = jnp.tile(lax.dynamic_slice_in_dim(sinks, kv_head * groups, groups, 0), row_total)
        row_max = jnp.maximum(sink_rows, jnp.maximum(jnp.max(score_cache, axis=1), jnp.max(score_tree, axis=1)))
        weight_cache = jnp.exp(score_cache - row_max[:, None])
        weight_tree = jnp.exp(score_tree - row_max[:, None])
        denominator = jnp.exp(sink_rows - row_max) + jnp.sum(weight_cache, axis=1) + jnp.sum(weight_tree, axis=1)
        numerator = jnp.dot(weight_cache.astype(jnp.bfloat16), value_cache, preferred_element_type=jnp.float32)
        numerator = numerator + jnp.dot(weight_tree.astype(jnp.bfloat16), value_tree, preferred_element_type=jnp.float32)
        return (numerator / denominator[:, None]).reshape(row_total, head_width)

    per_head = lax.map(per_kv_head, jnp.arange(KVH, dtype=jnp.int32))
    return jnp.transpose(per_head, (1, 0, 2)).reshape(row_total, QH * HD)


def reference(q_nodes, k_cache, v_cache, k_tree, v_tree, anc_bits, node_count, cache_len, sinks, o_weight):
    def per_request(request):
        queries, cache_keys, cache_values, tree_keys, tree_values, bit_words, node_limit, cache_count = request
        result = attend_rows(queries, unpack_bits(bit_words), cache_keys, cache_values, tree_keys, tree_values, cache_count, sinks)
        node_live = jnp.arange(queries.shape[0], dtype=jnp.int32) < node_limit
        attended_rows = jnp.where(node_live[:, None], result, jnp.zeros_like(result)).astype(jnp.bfloat16)
        projected_rows = jnp.dot(attended_rows, o_weight, preferred_element_type=jnp.float32).astype(jnp.bfloat16)
        return attended_rows, projected_rows

    attended, projected = lax.map(per_request, (q_nodes, k_cache, v_cache, k_tree, v_tree, anc_bits, node_count, cache_len))
    return (attended, projected)
```

```python
import functools

import jax
import jax.numpy as jnp
from jax import lax
from jax.experimental import pallas as pl
from jax.experimental.pallas import tpu as pltpu
from jax.sharding import PartitionSpec as P

KVH = 8
HD = 64
BLK = 128
MASKED = -1e30
AXES = ("gx", "gy")
VMEM_LIMIT = 60 * 1024 * 1024


def contract_last(a, b):
    return lax.dot_general(a, b, (((1,), (1,)), ((), ())), preferred_element_type=jnp.float32)


def attend_kernel(scal, q_ref, kc_ref, vc_ref, kt_ref, vt_ref, bias_ref, sink_ref, *rest):
    out_ref, kx, vx, qx = rest[-4:]
    head = pl.program_id(0)
    block = pl.program_id(1)
    cache_rows = kc_ref.shape[0]
    key_rows = kx.shape[0]
    groups = q_ref.shape[1] // HD

    @pl.when(block == 0)
    def _():
        src = lax.broadcasted_iota(jnp.int32, (BLK, BLK), 0)
        dst = lax.broadcasted_iota(jnp.int32, (BLK, BLK), 1)
        pick = jnp.where(src == (head % 2) * HD + dst % HD, 1.0, 0.0).astype(jnp.bfloat16)

        def both(x):
            return jnp.dot(x, pick, preferred_element_type=jnp.float32).astype(jnp.bfloat16)

        kx[0:cache_rows, 0:BLK] = both(kc_ref[...])
        kx[cache_rows:key_rows, 0:BLK] = both(kt_ref[...])
        vx[0:cache_rows, 0:BLK] = both(vc_ref[...])
        vx[cache_rows:key_rows, 0:BLK] = both(vt_ref[...])
        vx[:, BLK : 2 * BLK] = jnp.ones((key_rows, BLK), jnp.bfloat16)
        row = lax.broadcasted_iota(jnp.int32, (cache_rows, BLK), 0)
        kx[0:cache_rows, BLK : 2 * BLK] = jnp.where(row < scal[2], 0.0, MASKED).astype(jnp.bfloat16)
        own = jnp.where(src == dst, 1.0, 0.0).astype(jnp.bfloat16)
        for g in range(groups):
            qx[g * BLK : (g + 1) * BLK, BLK : 2 * BLK] = own

    live = block * BLK < scal[1]

    @pl.when(live)
    def _():
        kx[cache_rows:key_rows, BLK : 2 * BLK] = bias_ref[...]
        lane = lax.broadcasted_iota(jnp.int32, (BLK, BLK), 1)
        low = lane < HD
        node = lax.broadcasted_iota(jnp.int32, (BLK, BLK), 0) + block * BLK
        top = lax.broadcasted_iota(jnp.int32, (2 * BLK, 1), 0) < BLK
        zero = jnp.zeros((BLK, BLK), jnp.float32)
        for pair in range(groups // 2):
            cols = slice(pair * BLK, (pair + 1) * BLK)
            q2 = q_ref[:, cols].astype(jnp.float32) * (HD**-0.5)
            qx[(2 * pair) * BLK : (2 * pair + 1) * BLK, 0:BLK] = jnp.where(low, q2, zero).astype(
                jnp.bfloat16
            )
            qx[(2 * pair + 1) * BLK : (2 * pair + 2) * BLK, 0:BLK] = jnp.where(
                low, zero, q2
            ).astype(jnp.bfloat16)
        for pair in range(groups // 2):
            cols = slice(pair * BLK, (pair + 1) * BLK)
            rows = slice(2 * pair * BLK, (2 * pair + 2) * BLK)
            scores = contract_last(qx[rows, :], kx[...])
            sink = jnp.where(top, sink_ref[head * groups + 2 * pair], sink_ref[head * groups + 2 * pair + 1])
            peak = jnp.maximum(jnp.max(scores, axis=1, keepdims=True), sink)
            weights = jnp.exp(scores - peak).astype(jnp.bfloat16)
            sums = jnp.dot(weights, vx[...], preferred_element_type=jnp.float32)
            result = sums[:, 0:BLK] / (sums[:, BLK : 2 * BLK] + jnp.exp(sink - peak))
            joined = jnp.where(low, result[0:BLK], result[BLK : 2 * BLK])
            out_ref[:, cols] = jnp.where(node < scal[1], joined, zero).astype(out_ref.dtype)

    @pl.when(jnp.logical_not(live))
    def _():
        out_ref[...] = jnp.zeros_like(out_ref)


def attend(scal, q, k_cache, v_cache, k_tree, v_tree, bias, sinks, first, count, own, after):
    (q_arr, k_arr, v_arr, kt_arr, vt_arr), offsets, sizes = (
        (q, k_cache, v_cache, k_tree, v_tree),
        own["rows"],
        own["sizes"],
    )
    node_total = q_arr.shape[0]
    width = sinks.shape[0] // KVH * HD
    half = KVH // 2
    cache_rows, tree_rows = sizes
    whole = own["whole"]

    def col(s, h, per):
        base = s[0] * (half // per) if whole else 0
        return base + (first + h) // per

    def kv_spec(rows, at):
        return pl.BlockSpec((rows, BLK), lambda h, i, s: (at, col(s, h, 2)))

    grid_spec = pltpu.PrefetchScalarGridSpec(
        num_scalar_prefetch=1,
        grid=(count, node_total // BLK),
        in_specs=[
            pl.BlockSpec((BLK, width), lambda h, i, s: (i, col(s, h, 1))),
            kv_spec(cache_rows, offsets[0]),
            kv_spec(cache_rows, offsets[1]),
            kv_spec(tree_rows, offsets[2]),
            kv_spec(tree_rows, offsets[3]),
            pl.BlockSpec((tree_rows, BLK), lambda h, i, s: (0, i)),
            pl.BlockSpec(memory_space=pltpu.SMEM),
        ]
        + [pl.BlockSpec(memory_space=pl.ANY)] * len(after),
        out_specs=pl.BlockSpec((BLK, width), lambda h, i, s: (i, h)),
        scratch_shapes=[
            pltpu.VMEM((cache_rows + tree_rows, 2 * BLK), jnp.bfloat16),
            pltpu.VMEM((cache_rows + tree_rows, 2 * BLK), jnp.bfloat16),
            pltpu.VMEM((width // HD * BLK, 2 * BLK), jnp.bfloat16),
        ],
    )
    groups = width // HD
    keys = cache_rows + tree_rows
    rows = count * groups * node_total // 2
    half_sinks = lax.dynamic_slice(
        sinks, (scal[0] * (half * groups) + first * groups,), (count * groups,)
    )
    return pl.pallas_call(
        attend_kernel,
        grid_spec=grid_spec,
        out_shape=jax.ShapeDtypeStruct((node_total, count * width), jnp.bfloat16),
        compiler_params=pltpu.CompilerParams(vmem_limit_bytes=VMEM_LIMIT),
        cost_estimate=pl.CostEstimate(
            flops=rows * keys * 2 * 512,
            bytes_accessed=4 * keys * BLK * 2,
            transcendentals=rows * keys,
        ),
        name="attend",
    )(scal, q_arr, k_arr, v_arr, kt_arr, vt_arr, bias, half_sinks, *after)


def tree_bias(words_t, key_total):
    spread = jnp.repeat(words_t, 32, axis=0)
    shift = (jnp.arange(key_total, dtype=jnp.int32) % 32)[:, None]
    flag = jnp.bitwise_and(lax.shift_right_logical(spread, jnp.broadcast_to(shift, spread.shape)), 1)
    return jnp.where(flag > 0, 0.0, MASKED).astype(jnp.bfloat16)


def project_kernel(plan, last, has_acc, info, busy_ref, light_ref, *refs):
    refs = list(refs)
    acc_in = refs.pop(0) if has_acc else None
    blocks = refs[: len(plan)]
    refs = refs[len(plan) :]
    if last:
        own_ref, other_ref, acc = refs
    else:
        (acc,) = refs
    busy_rows = busy_ref.shape[0]
    light_rows = light_ref.shape[0]
    if has_acc:
        acc[...] = acc_in[...]
    started = has_acc
    for at, (slot, low, high) in enumerate(plan):
        block = blocks[at][...]
        depth = block.shape[1]
        cols = pl.ds(pl.multiple_of(info[slot] * depth, depth), depth)
        for x_ref, base, rows in ((busy_ref, 0, busy_rows), (light_ref, busy_rows, light_rows)):
            part = contract_last(x_ref[:, cols], block)
            where = (slice(base, base + rows), slice(low, high))
            if started:
                acc[where] += part
            else:
                acc[where] = part
        started = True
    if last:
        done = acc[...].astype(jnp.bfloat16)
        busy, light = done[:busy_rows], done[busy_rows:]
        rest = jnp.zeros((busy_rows - light_rows, done.shape[1]), jnp.bfloat16)

        @pl.when(info[len(info_slots())] > 0)
        def _():
            own_ref[...] = busy
            other_ref[0:light_rows, :] = light
            other_ref[light_rows:, :] = rest

        @pl.when(info[len(info_slots())] <= 0)
        def _():
            other_ref[...] = busy
            own_ref[0:light_rows, :] = light
            own_ref[light_rows:, :] = rest


def info_slots():
    return tuple(range(16))


def project(info, busy, light, acc, blocks, plan, columns, last):
    rows = busy.shape[0] + light.shape[0]
    acc_shape = jax.ShapeDtypeStruct((rows, columns), jnp.float32)
    half = jax.ShapeDtypeStruct((busy.shape[0], columns), jnp.bfloat16)
    vmem = pl.BlockSpec(memory_space=pltpu.VMEM)
    operands = [info, busy, light] + ([] if acc is None else [acc]) + list(blocks)
    flops = sum(2 * rows * b.size for b in blocks)
    return pl.pallas_call(
        functools.partial(project_kernel, plan, last, acc is not None),
        out_shape=(half, half) if last else acc_shape,
        in_specs=[pl.BlockSpec(memory_space=pltpu.SMEM)] + [vmem] * (len(operands) - 1),
        out_specs=(vmem, vmem) if last else vmem,
        scratch_shapes=[pltpu.VMEM((rows, columns), jnp.float32)] if last else [],
        compiler_params=pltpu.CompilerParams(vmem_limit_bytes=VMEM_LIMIT),
        cost_estimate=pl.CostEstimate(flops=flops, bytes_accessed=rows * columns * 8, transcendentals=0),
        name="project",
    )(*operands)


def on_device(plane, line, args):
    (
        q_nodes, k_cache, v_cache, k_tree, v_tree, anc_bits, node_count, cache_len, sinks, o_weight,
    ) = args
    gx = lax.axis_index("gx")
    gy = lax.axis_index("gy")
    core = gy % 2
    z = gy // 2
    places = [(a, b, c) for a in range(plane) for b in range(line) for c in range(2)]

    def number(a, b, c):
        return (a * line + b) * 2 + c

    def moved(x, to):
        pairs = [(number(*p), number(*to(*p))) for p in places]
        return lax.ppermute(x, AXES, pairs)

    def swapped(x):
        return moved(x, lambda a, b, c: (a, b, 1 - c))

    q, kc, vc, kt, vt = q_nodes[0], k_cache[0], v_cache[0], k_tree[0], v_tree[0]
    node_total = q.shape[0]
    cache_rows, tree_rows = kc.shape[0], kt.shape[0]
    columns = o_weight.shape[1] // 2
    half_q, half_kv = q.shape[1] // 2, kc.shape[1] // 2
    far = 1 - core

    w_t = o_weight.T
    w_mine = lax.dynamic_slice_in_dim(w_t, core * columns, columns, 0)
    w_theirs = swapped(lax.dynamic_slice_in_dim(w_t, far * columns, columns, 0))
    own_block = jnp.where(
        core == 0,
        jnp.concatenate([w_mine, w_theirs], axis=1),
        jnp.concatenate([w_theirs, w_mine], axis=1),
    )

    words_t = anc_bits[0].T
    counts = jnp.concatenate([node_count, cache_len])
    note = jnp.concatenate([words_t, jnp.broadcast_to(counts[:, None], (2, node_total))], axis=0)
    q_away = lax.dynamic_slice_in_dim(q, far * half_q, half_q, 1)
    kv_away = jnp.concatenate(
        [lax.dynamic_slice_in_dim(a, far * half_kv, half_kv, 1) for a in (kc, vc, kt, vt)], axis=0
    )
    q_got, kv_got, note_got = swapped(q_away), swapped(kv_away), swapped(note)

    bias = tree_bias(words_t, tree_rows)
    scal = jnp.stack([core, node_count[0], cache_len[0]]).astype(jnp.int32)
    own = dict(rows=(0, 0, 0, 0), sizes=(cache_rows, tree_rows), whole=True)
    ratio = cache_rows // tree_rows
    got = dict(rows=(0, 1, 2 * ratio, 2 * ratio + 1), sizes=(cache_rows, tree_rows), whole=False)
    word_total = words_t.shape[0]
    bias_got = tree_bias(note_got[:word_total], tree_rows)
    scal_got = jnp.stack([core, note_got[word_total, 0], note_got[word_total + 1, 0]]).astype(jnp.int32)

    def attend_own(first, after):
        return attend(scal, q, kc, vc, kt, vt, bias, sinks, first, KVH // 4, own, after)

    def attend_got(first, after):
        return attend(
            scal_got, q_got, kv_got, kv_got, kv_got, kv_got, bias_got, sinks, first, KVH // 4, got, after
        )

    chips = plane * line
    direct = plane == 4 and line == 4

    if direct:
        def along_x(x):
            return moved(x, lambda a, b, c: (a ^ 1, b, c))

        def along_y(x):
            return moved(x, lambda a, b, c: (a ^ 2, b, c))

        def along_z(x, by):
            return moved(x, lambda a, b, c: (a, (b + by) % line, c))

        cut = columns // (2 * BLK) * BLK + BLK
        b0 = own_block
        x0, y0 = along_x(b0), along_y(b0)
        z1, z3, z2 = along_z(b0, 1), along_z(b0, 3), along_z(b0, 2)

        def diagonal(xk, yk):
            return along_x(yk[:cut]), along_y(xk[cut:])

        mine01 = attend_own(0, ())
        d0 = diagonal(x0, y0)
        x1, y1 = along_x(z1), along_y(z1)
        theirs01 = attend_got(0, (x0, y0, z1))
        d1 = diagonal(x1, y1)
        x3, y3 = along_x(z3), along_y(z3)
        mine23 = attend_own(KVH // 4, (x1, y1, z3, *d0))
        theirs23 = attend_got(KVH // 4, (x1, y1, z3, *d0))
        d3 = diagonal(x3, y3)
        x2, y2 = along_x(z2), along_y(z2)
        d2 = diagonal(x2, y2)
    else:
        mine01 = attend_own(0, ())
        theirs01 = attend_got(0, ())
        mine23 = attend_own(KVH // 4, ())
        theirs23 = attend_got(KVH // 4, ())

    mine = jnp.concatenate([mine01, mine23], axis=1)
    theirs = jnp.concatenate([theirs01, theirs23], axis=1)
    mine_back = jnp.concatenate([swapped(theirs01), swapped(theirs23)], axis=1)
    theirs_own = jnp.concatenate([swapped(mine01), swapped(mine23)], axis=1)

    def in_order(here, there):
        return jnp.where(
            core == 0,
            jnp.concatenate([here, there], axis=1),
            jnp.concatenate([there, here], axis=1),
        )

    attended = in_order(mine, mine_back)
    other = in_order(theirs, theirs_own)
    is_busy = (gx + gy) % 2 == 0
    busy = jnp.where(is_busy, attended, other)
    light = jnp.where(is_busy, other[:BLK], attended[:BLK])

    if direct:
        places_of = {}
        slots = []
        for dz in (0, 1, 3, 2):
            for flip in (0, 1, 2, 3):
                places_of[(dz, flip)] = len(slots)
                slots.append((gx ^ flip) * line + (z - dz) % line)
        info = jnp.stack(slots + [is_busy.astype(jnp.int32)]).astype(jnp.int32)

        def whole(dz, flip):
            return (places_of[(dz, flip)], 0, columns)

        def halves(dz):
            at = places_of[(dz, 3)]
            return [(at, 0, cut), (at, cut, columns)]

        early = [b0, x0, y0, z1, x1, y1, *d0]
        early_plan = [whole(0, 0), whole(0, 1), whole(0, 2), whole(1, 0), whole(1, 1), whole(1, 2)]
        early_plan += halves(0)
        acc = project(info, busy, light, None, early, early_plan, columns, False)
        late = [z3, x3, y3, *d1, z2]
        late_plan = [whole(3, 0), whole(3, 1), whole(3, 2), *halves(1), whole(2, 0)]
        acc = project(info, busy, light, acc, late, late_plan, columns, False)
        end = [x2, y2, *d3, *d2]
        end_plan = [whole(2, 1), whole(2, 2), *halves(3), *halves(2)]
        own_half, other_half = project(info, busy, light, acc, end, end_plan, columns, True)
    else:
        w_all = lax.all_gather(o_weight, AXES, axis=0, tiled=True)
        w_half = lax.dynamic_slice_in_dim(w_all, core * columns, columns, 1)

        def dot(x):
            return jnp.dot(x, w_half, preferred_element_type=jnp.float32).astype(jnp.bfloat16)

        own_half, other_half = dot(attended), dot(other)

    projected = in_order(own_half, swapped(other_half))
    return attended[None], projected[None]


def solution(mesh):
    plane, line = mesh.shape["gx"], mesh.shape["gy"] // 2
    rows = P(AXES, None, None)
    placed = (rows, rows, rows, rows, rows, rows, P(AXES), P(AXES), P(), P(AXES, None))

    def run(*args):
        return on_device(plane, line, args)

    return jax.shard_map(run, mesh=mesh, in_specs=placed, out_specs=(rows, rows), check_vma=False)
```

```python
import functools

import jax
import jax.numpy as jnp
from jax import lax
from jax.experimental import pallas as pl
from jax.experimental.pallas import tpu as pltpu
from jax.sharding import PartitionSpec as P

KVH = 8
HD = 64
BLK = 128
MASKED = -1e30
TRUSTED = 1e26
AXES = ("gx", "gy")
VMEM_LIMIT = 60 * 1024 * 1024


def contract_last(a, b):
    return lax.dot_general(a, b, (((1,), (1,)), ((), ())), preferred_element_type=jnp.float32)


def dot(a, b):
    return jnp.dot(a, b, preferred_element_type=jnp.float32)


def attend_kernel(chained, first, scal, *refs):
    here, there = refs[0:6], refs[6:12]
    sink_ref = refs[12]
    big_ref, piece_ref, kx, vx, qx, worst = refs[13 + chained :]
    block = pl.program_id(0) + first
    use_here = scal[3] > 0
    cache_rows, tree_rows = here[1].shape[0], here[3].shape[0]
    key_rows = cache_rows + tree_rows
    pairs = here[0].shape[1] // BLK // 2
    node_total = jnp.where(use_here, scal[1], scal[4])
    cache_total = jnp.where(use_here, scal[2], scal[5])

    def chosen(source):
        _, kc_ref, vc_ref, kt_ref, vt_ref, _ = source
        kx[0:cache_rows, 0:BLK] = kc_ref[...]
        kx[cache_rows:key_rows, 0:BLK] = kt_ref[...]
        vx[0:cache_rows, 0:BLK] = vc_ref[...]
        vx[cache_rows:key_rows, 0:BLK] = vt_ref[...]

    @pl.when(block == first)
    def _():
        @pl.when(use_here)
        def _():
            chosen(here)

        @pl.when(jnp.logical_not(use_here))
        def _():
            chosen(there)

        vx[:, BLK : 2 * BLK] = jnp.ones((key_rows, BLK), jnp.bfloat16)
        row = lax.broadcasted_iota(jnp.int32, (cache_rows, BLK), 0)
        kx[0:cache_rows, BLK : 2 * BLK] = jnp.where(row < cache_total, 0.0, MASKED).astype(jnp.bfloat16)
        src = lax.broadcasted_iota(jnp.int32, (BLK, BLK), 0)
        dst = lax.broadcasted_iota(jnp.int32, (BLK, BLK), 1)
        own = jnp.where(src == dst, 1.0, 0.0).astype(jnp.bfloat16)
        for at in range(qx.shape[0]):
            qx[at, 0:BLK, BLK : 2 * BLK] = own
            qx[at, BLK : 2 * BLK, BLK : 2 * BLK] = own

    live = block * BLK < node_total

    @pl.when(live)
    def _():
        lane = lax.broadcasted_iota(jnp.int32, (BLK, BLK), 1)
        low = lane < HD
        node = lax.broadcasted_iota(jnp.int32, (BLK, BLK), 0) + block * BLK
        top = lax.broadcasted_iota(jnp.int32, (2 * BLK, 1), 0) < BLK
        zero = jnp.zeros((BLK, BLK), jnp.float32)
        kx[cache_rows:key_rows, BLK : 2 * BLK] = jnp.where(use_here, here[5][...], there[5][...])

        def queries(head, pair):
            cols = pl.ds(pl.multiple_of((head * pairs + pair) * BLK, BLK), BLK)
            both = jnp.where(use_here, here[0][:, cols], there[0][:, cols]).astype(jnp.float32) * (HD**-0.5)
            turned = pltpu.roll(both, HD, 1)
            if head == 0:
                first, second = jnp.where(low, both, zero), jnp.where(low, turned, zero)
            else:
                first, second = jnp.where(low, zero, turned), jnp.where(low, zero, both)
            qx[head, 0:BLK, 0:BLK] = first.astype(jnp.bfloat16)
            qx[head, BLK : 2 * BLK, 0:BLK] = second.astype(jnp.bfloat16)
            return qx[head]

        def sink_of(head, pair, kind):
            at = 2 * (head * pairs + pair)
            return jnp.where(top, sink_ref[kind, at], sink_ref[kind, at + 1])

        def store(head, pair, result):
            first, second = result[0:BLK], result[BLK : 2 * BLK]
            if head == 0:
                joined = jnp.where(low, first, pltpu.roll(second, HD, 1))
            else:
                joined = jnp.where(low, pltpu.roll(first, HD, 1), second)
            joined = jnp.where(node < node_total, joined, zero).astype(jnp.bfloat16)
            cols = pl.ds(pl.multiple_of((head * pairs + pair) * BLK, BLK), BLK)
            big_ref[:, cols] = joined
            piece_ref[:, cols] = joined

        worst[...] = zero

        def quick(pair, carry):
            for head in (0, 1):
                scores = contract_last(queries(head, pair), kx[...])
                weights = jnp.exp(scores).astype(jnp.bfloat16)
                sums = dot(weights, vx[...])
                under = sums[:, BLK : 2 * BLK] + sink_of(head, pair, 1)
                worst[...] = jnp.maximum(worst[...], jnp.maximum(under[0:BLK], under[BLK : 2 * BLK]))
                store(head, pair, sums[:, 0:BLK] / under)
            return carry

        lax.fori_loop(0, pairs, quick, 0)

        @pl.when(jnp.logical_not(jnp.max(worst[...]) < TRUSTED))
        def _():
            def careful(pair, carry):
                for head in (0, 1):
                    scores = contract_last(queries(head, pair), kx[...])
                    sink = sink_of(head, pair, 0)
                    peak = jnp.maximum(jnp.max(scores, axis=1, keepdims=True), sink)
                    weights = jnp.exp(scores - peak).astype(jnp.bfloat16)
                    sums = dot(weights, vx[...])
                    under = sums[:, BLK : 2 * BLK] + jnp.exp(sink - peak)
                    store(head, pair, sums[:, 0:BLK] / under)
                return carry

            lax.fori_loop(0, pairs, careful, 0)

    @pl.when(jnp.logical_not(live))
    def _():
        big_ref[...] = jnp.zeros_like(big_ref)
        piece_ref[...] = jnp.zeros_like(piece_ref)


def attend(scal, here, there, sinks, at, first, count, rows, tree_rows, before):
    q, k_cache, _, k_tree, _, _ = here
    q_got, kv_got, bias_got = there
    cache_rows = k_cache.shape[0]
    width = q.shape[1] // (KVH // 2)
    full_tree = k_tree.shape[0]
    first_tree = 2 * cache_rows // tree_rows
    second_tree = (2 * cache_rows + full_tree) // tree_rows
    keys = cache_rows + tree_rows
    per_core = KVH // 4

    def mine(s):
        return s[0] * per_core + at

    in_specs = [
        pl.BlockSpec((BLK, width), lambda i, s: (first + i, mine(s))),
        *[pl.BlockSpec((cache_rows, BLK), lambda i, s: (0, mine(s)))] * 2,
        *[pl.BlockSpec((tree_rows, BLK), lambda i, s: (0, mine(s)))] * 2,
        pl.BlockSpec((tree_rows, BLK), lambda i, s: (0, first + i)),
        pl.BlockSpec((BLK, width), lambda i, s: (first + i, at)),
        pl.BlockSpec((cache_rows, BLK), lambda i, s: (0, at)),
        pl.BlockSpec((cache_rows, BLK), lambda i, s: (1, at)),
        pl.BlockSpec((tree_rows, BLK), lambda i, s: (first_tree, at)),
        pl.BlockSpec((tree_rows, BLK), lambda i, s: (second_tree, at)),
        pl.BlockSpec((tree_rows, BLK), lambda i, s: (0, first + i)),
        pl.BlockSpec(memory_space=pltpu.SMEM),
    ]
    operands = [*here, q_got, kv_got, kv_got, kv_got, kv_got, bias_got, sinks]
    aliases = {}
    for out, array in enumerate(before):
        if array is not None:
            aliases[1 + len(operands)] = out
            in_specs.append(pl.BlockSpec(memory_space=pl.ANY))
            operands.append(array)
    heads = width // HD
    work = count * BLK * heads * keys
    return pl.pallas_call(
        functools.partial(attend_kernel, len(aliases), first),
        grid_spec=pltpu.PrefetchScalarGridSpec(
            num_scalar_prefetch=1,
            grid=(count,),
            in_specs=in_specs,
            out_specs=[
                pl.BlockSpec((BLK, width), lambda i, s: (first + i, mine(s))),
                pl.BlockSpec((BLK, width), lambda i, s: (first + i, 0)),
            ],
            scratch_shapes=[
                pltpu.VMEM((keys, 2 * BLK), jnp.bfloat16),
                pltpu.VMEM((keys, 2 * BLK), jnp.bfloat16),
                pltpu.VMEM((2, 2 * BLK, 2 * BLK), jnp.bfloat16),
                pltpu.VMEM((BLK, BLK), jnp.float32),
            ],
        ),
        out_shape=[
            jax.ShapeDtypeStruct((rows, q.shape[1]), jnp.bfloat16),
            jax.ShapeDtypeStruct((rows, width), jnp.bfloat16),
        ],
        input_output_aliases=aliases,
        compiler_params=pltpu.CompilerParams(vmem_limit_bytes=VMEM_LIMIT),
        cost_estimate=pl.CostEstimate(
            flops=work * 2 * 4 * BLK, bytes_accessed=8 * keys * BLK, transcendentals=work
        ),
        name="attend",
    )(scal, *operands)


def tree_bias(words_t, key_total):
    spread = jnp.repeat(words_t, 32, axis=0)
    shift = (jnp.arange(key_total, dtype=jnp.int32) % 32)[:, None]
    flag = jnp.bitwise_and(lax.shift_right_logical(spread, jnp.broadcast_to(shift, spread.shape)), 1)
    return jnp.where(flag > 0, 0.0, MASKED).astype(jnp.bfloat16)


def project_kernel(slots, last, has_acc, info, *refs):
    refs = list(refs)
    n = len(slots)
    busy, light, blocks = refs[:n], refs[n : 2 * n], refs[2 * n : 3 * n]
    refs = refs[3 * n :]
    part = None
    for x in range(n):
        rows = jnp.concatenate([busy[x][...], light[x][...]], axis=0)
        term = contract_last(blocks[x][...], rows)
        part = term if part is None else part + term
    if has_acc:
        part = part + refs.pop(0)[...]
    if not last:
        refs[0][...] = part
        return
    own_ref, other_ref = refs
    done = part.astype(jnp.bfloat16)
    nodes = busy[0].shape[0]
    few = light[0].shape[0]
    rest = jnp.zeros((done.shape[0], nodes - few), jnp.bfloat16)

    @pl.when(info[0] > 0)
    def _():
        own_ref[...] = done[:, :nodes]
        other_ref[:, 0:few] = done[:, nodes:]
        other_ref[:, few:] = rest

    @pl.when(info[0] <= 0)
    def _():
        other_ref[...] = done[:, :nodes]
        own_ref[:, 0:few] = done[:, nodes:]
        own_ref[:, few:] = rest


def project(info, busy, light, acc, blocks, slots, last):
    columns, depth = blocks[0].shape
    tile = columns // 6
    rows = busy.shape[0] + light.shape[0]
    n = len(slots)

    def at_slot(rows_of, slot):
        return pl.BlockSpec((rows_of, depth), lambda i, s: (0, s[slot]))

    in_specs = [at_slot(busy.shape[0], slot) for slot in slots]
    in_specs += [at_slot(light.shape[0], slot) for slot in slots]
    in_specs += [pl.BlockSpec((tile, depth), lambda i, s: (i, 0))] * n
    operands = [busy] * n + [light] * n + list(blocks)
    if acc is not None:
        in_specs.append(pl.BlockSpec((tile, rows), lambda i, s: (i, 0)))
        operands.append(acc)
    if last:
        out_specs = [
            pl.BlockSpec((tile, busy.shape[0]), lambda i, s: (s[1] * 6 + i, 0)),
            pl.BlockSpec((tile, busy.shape[0]), lambda i, s: (i, 0)),
        ]
        out_shape = [
            jax.ShapeDtypeStruct((2 * columns, busy.shape[0]), jnp.bfloat16),
            jax.ShapeDtypeStruct((columns, busy.shape[0]), jnp.bfloat16),
        ]
    else:
        out_specs = pl.BlockSpec((tile, rows), lambda i, s: (i, 0))
        out_shape = jax.ShapeDtypeStruct((columns, rows), jnp.float32)
    return pl.pallas_call(
        functools.partial(project_kernel, slots, last, acc is not None),
        grid_spec=pltpu.PrefetchScalarGridSpec(
            num_scalar_prefetch=1, grid=(6,), in_specs=in_specs, out_specs=out_specs
        ),
        out_shape=out_shape,
        compiler_params=pltpu.CompilerParams(vmem_limit_bytes=VMEM_LIMIT),
        cost_estimate=pl.CostEstimate(
            flops=2 * rows * columns * depth * n, bytes_accessed=rows * columns * 8, transcendentals=0
        ),
        name="project",
    )(info, *operands)


def on_device(plane, line, args):
    (
        q_nodes, k_cache, v_cache, k_tree, v_tree, anc_bits, node_count, cache_len, sinks, o_weight,
    ) = args
    gx = lax.axis_index("gx")
    gy = lax.axis_index("gy")
    core = gy % 2
    far = 1 - core
    z = gy // 2
    is_busy = (gx + gy) % 2 == 0
    places = [(a, b, c) for a in range(plane) for b in range(line) for c in range(2)]

    def number(a, b, c):
        return (a * line + b) * 2 + c

    def moved(x, to):
        pairs = [(number(*p), number(*to(*p))) for p in places]
        return lax.ppermute(x, AXES, pairs)

    def swapped(x):
        return moved(x, lambda a, b, c: (a, b, 1 - c))

    q, kc, vc, kt, vt = q_nodes[0], k_cache[0], v_cache[0], k_tree[0], v_tree[0]
    node_total = q.shape[0]
    tree_rows = kt.shape[0]
    columns = o_weight.shape[1] // 2
    half_q, half_kv = q.shape[1] // 2, kc.shape[1] // 2

    w_t = o_weight.T
    w_mine = lax.dynamic_slice_in_dim(w_t, core * columns, columns, 0)
    w_theirs = swapped(lax.dynamic_slice_in_dim(w_t, far * columns, columns, 0))
    b0 = jnp.where(
        core == 0,
        jnp.concatenate([w_mine, w_theirs], axis=1),
        jnp.concatenate([w_theirs, w_mine], axis=1),
    )

    words_t = anc_bits[0].T
    counts = jnp.concatenate([node_count, cache_len])
    note = jnp.concatenate([words_t, jnp.broadcast_to(counts[:, None], (2, node_total))], axis=0)
    q_away = lax.dynamic_slice_in_dim(q, far * half_q, half_q, 1)
    kv_away = jnp.concatenate(
        [lax.dynamic_slice_in_dim(a, far * half_kv, half_kv, 1) for a in (kc, vc, kt, vt)], axis=0
    )
    q_got, kv_got, note_got = swapped(q_away), swapped(kv_away), swapped(note)
    words = words_t.shape[0]
    here = (q, kc, vc, kt, vt, tree_bias(words_t, tree_rows))
    there = (q_got, kv_got, tree_bias(note_got[:words], tree_rows))
    numbers = [node_count[0], cache_len[0], note_got[words, 0], note_got[words + 1, 0]]

    def scalars(use_here):
        flag = use_here.astype(jnp.int32)
        return jnp.stack([core, numbers[0], numbers[1], flag, numbers[2], numbers[3]]).astype(jnp.int32)

    per_pair = sinks.shape[0] // 4
    sink_table = jnp.stack([sinks, jnp.exp(sinks)])

    def pair_sinks(at):
        return lax.dynamic_slice_in_dim(sink_table, (core * 2 + at) * per_pair, per_pair, 1)

    half = node_total // BLK // 2

    def attend_busy(at, first, before):
        flags = scalars(is_busy)
        return attend(
            flags, here, there, pair_sinks(at), at, first, half, node_total, tree_rows, before
        )

    def attend_light(at, big):
        flags = scalars(jnp.logical_not(is_busy))
        return attend(flags, here, there, pair_sinks(at), at, 0, 1, BLK, BLK, (big, None))

    direct = plane == 4 and line == 4

    def along_x(x):
        return moved(x, lambda a, b, c: (a ^ 1, b, c))

    def along_y(x):
        return moved(x, lambda a, b, c: (a ^ 2, b, c))

    def along_z(x, by):
        return moved(x, lambda a, b, c: (a, (b + by) % line, c))

    def together(*arrays):
        return lax.optimization_barrier(arrays) if direct else arrays

    if direct:
        x0, y0, z1 = along_x(b0), along_y(b0), along_z(b0, 1)
    else:
        x0 = y0 = z1 = b0
    busy, busy0 = attend_busy(0, 0, (None, None))
    busy, busy0, b0, x0, y0, z1 = together(busy, busy0, b0, x0, y0, z1)
    if direct:
        d0, y1, z3 = along_x(y0), along_y(z1), along_z(b0, 3)
        x1, z2 = along_x(z1), along_z(z1, 1)
    else:
        d0 = y1 = z3 = x1 = z2 = b0
    busy, busy0 = attend_busy(0, half, (busy, busy0))
    busy, busy0, d0, y1, z3 = together(busy, busy0, d0, y1, z3)
    if direct:
        y3, d1, d3 = along_y(z3), along_z(d0, 1), along_z(d0, 3)
    else:
        y3 = d1 = d3 = b0
    busy, busy1 = attend_busy(1, 0, (busy, None))
    busy, busy1, x1, z2, z3 = together(busy, busy1, x1, z2, z3)
    if direct:
        x2, y2, x3 = along_x(z2), along_y(z2), along_x(z3)
    else:
        x2 = y2 = x3 = b0
    busy, busy1 = attend_busy(1, half, (busy, busy1))
    busy, busy1, x2 = together(busy, busy1, x2)
    d2 = along_y(x2) if direct else b0
    light, light0 = attend_light(0, None)
    light, light1 = attend_light(1, light)
    for at, (piece_b, piece_l) in enumerate(((busy0, light0), (busy1, light1))):
        col = (far * 2 + at) * busy0.shape[1]
        busy = lax.dynamic_update_slice(busy, swapped(piece_b), (0, col))
        light = lax.dynamic_update_slice(light, swapped(piece_l), (0, col))

    padded = jnp.concatenate([light, jnp.zeros((node_total - BLK, light.shape[1]), light.dtype)], axis=0)
    attended = jnp.where(is_busy, busy, padded)

    if direct:
        slots = {}
        info = [is_busy.astype(jnp.int32), core]
        for dz in (0, 1, 3, 2):
            for flip in (0, 1, 2, 3):
                slots[(dz, flip)] = len(info)
                info.append((gx ^ flip) * line + (z - dz) % line)
        info = jnp.stack(info).astype(jnp.int32)

        def stage(acc, blocks, last):
            return project(
                info, busy, light, acc, [b for b, _ in blocks], tuple(slots[k] for _, k in blocks), last
            )

        blocks = [
            (b0, (0, 0)), (x0, (0, 1)), (y0, (0, 2)), (d0, (0, 3)),
            (z1, (1, 0)), (x1, (1, 1)), (y1, (1, 2)), (d1, (1, 3)),
            (z3, (3, 0)), (x3, (3, 1)), (y3, (3, 2)), (d3, (3, 3)),
            (z2, (2, 0)), (x2, (2, 1)), (y2, (2, 2)), (d2, (2, 3)),
        ]
        full, other_half = stage(None, blocks, True)
        full = lax.dynamic_update_slice(full, swapped(other_half), (far * columns, 0))
        projected = full.T
    else:
        w_all = lax.all_gather(o_weight, AXES, axis=0, tiled=True)
        projected = dot(attended, w_all).astype(jnp.bfloat16)
    return attended[None], projected[None]


def solution(mesh):
    plane, line = mesh.shape["gx"], mesh.shape["gy"] // 2
    rows = P(AXES, None, None)
    placed = (rows, rows, rows, rows, rows, rows, P(AXES), P(AXES), P(), P(AXES, None))

    def run(*args):
        return on_device(plane, line, args)

    return jax.shard_map(run, mesh=mesh, in_specs=placed, out_specs=(rows, rows), check_vma=False)
```

```python
import functools

import jax
import jax.numpy as jnp
from jax import lax
from jax.experimental import pallas as pl
from jax.experimental.pallas import tpu as pltpu
from jax.sharding import PartitionSpec as P

KVH = 8
HD = 64
BLK = 128
MASKED = -1e30
TRUSTED = 1e26
AXES = ("gx", "gy")
VMEM_LIMIT = 60 * 1024 * 1024


def contract_last(a, b):
    return lax.dot_general(a, b, (((1,), (1,)), ((), ())), preferred_element_type=jnp.float32)


def dot(a, b):
    return jnp.dot(a, b, preferred_element_type=jnp.float32)


def attend_kernel(for_busy, chained, first, at, scal, *refs):
    q_here, bias_here, q_there, bias_there = refs[0:4]
    here, there = refs[4:8], refs[8:12]
    sink_ref = refs[12]
    out_ref, kx_all, vx_all, qx, sums, arrived = refs[13 + chained :]
    step = pl.program_id(1)
    block = step + first
    here_busy = scal[3] > 0
    use_here = here_busy if for_busy else jnp.logical_not(here_busy)
    cache_rows = here[0].shape[0]
    key_rows = kx_all.shape[1]
    tree_rows = key_rows - cache_rows
    groups = q_here.shape[1] // HD // 2
    node_total = jnp.where(use_here, scal[1], scal[4])
    cache_total = jnp.where(use_here, scal[2], scal[5])
    which = pl.program_id(0)
    pairs = kx_all.shape[0]
    kx, vx = kx_all.at[which], vx_all.at[which]
    lane_pair = scal[0] * (KVH // 4) + at + which
    sink_base = lane_pair * (2 * groups)

    def loads(source, pair):
        cols = pl.ds(pl.multiple_of((scal[0] * (KVH // 4) + at + pair) * BLK, BLK), BLK)
        kc_ref, vc_ref, kt_ref, vt_ref = source
        low, high = pl.ds(0, cache_rows), pl.ds(cache_rows, tree_rows)
        lanes, tree = pl.ds(0, BLK), pl.ds(0, tree_rows)
        return (
            pltpu.make_async_copy(kc_ref.at[low, cols], kx_all.at[pair, low, lanes], arrived.at[pair, 0]),
            pltpu.make_async_copy(kt_ref.at[tree, cols], kx_all.at[pair, high, lanes], arrived.at[pair, 1]),
            pltpu.make_async_copy(vc_ref.at[low, cols], vx_all.at[pair, low, lanes], arrived.at[pair, 2]),
            pltpu.make_async_copy(vt_ref.at[tree, cols], vx_all.at[pair, high, lanes], arrived.at[pair, 3]),
        )

    @pl.when((step == 0) & (which == 0))
    def _():
        @pl.when(use_here)
        def _():
            for pair in range(pairs):
                for load in loads(here, pair):
                    load.start()

        @pl.when(jnp.logical_not(use_here))
        def _():
            for pair in range(pairs):
                for load in loads(there, pair):
                    load.start()

        row = lax.broadcasted_iota(jnp.int32, (cache_rows, BLK), 0)
        hidden = jnp.where(row < cache_total, 0.0, MASKED).astype(jnp.bfloat16)
        for pair in range(pairs):
            vx_all[pair, :, BLK : 2 * BLK] = jnp.ones((key_rows, BLK), jnp.bfloat16)
            kx_all[pair, 0:cache_rows, BLK : 2 * BLK] = hidden
        src = lax.broadcasted_iota(jnp.int32, (BLK, BLK), 0)
        dst = lax.broadcasted_iota(jnp.int32, (BLK, BLK), 1)
        own = jnp.where(src == dst, 1.0, 0.0).astype(jnp.bfloat16)
        for head in (0, 1):
            for g in range(groups):
                qx[head, g * BLK : (g + 1) * BLK, BLK : 2 * BLK] = own

    live = block * BLK < node_total
    lane = lax.broadcasted_iota(jnp.int32, (BLK, BLK), 1)
    low = lane < HD
    zero = jnp.zeros((BLK, BLK), jnp.float32)

    @pl.when(live)
    def _():
        kx[cache_rows:key_rows, BLK : 2 * BLK] = jnp.where(use_here, bias_here[...], bias_there[...])
        for head in (0, 1):
            for pair in range(groups // 2):
                cols = slice((head * groups // 2 + pair) * BLK, (head * groups // 2 + pair + 1) * BLK)
                both = jnp.where(use_here, q_here[:, cols], q_there[:, cols]).astype(jnp.float32) * (HD**-0.5)
                turned = pltpu.roll(both, HD, 1)
                if head == 0:
                    upper, lower = jnp.where(low, both, zero), jnp.where(low, turned, zero)
                else:
                    upper, lower = jnp.where(low, zero, turned), jnp.where(low, zero, both)
                at_row = 2 * pair * BLK
                qx[head, at_row : at_row + BLK, 0:BLK] = upper.astype(jnp.bfloat16)
                qx[head, at_row + BLK : at_row + 2 * BLK, 0:BLK] = lower.astype(jnp.bfloat16)

    @pl.when(step == 0)
    def _():
        for load in loads(here, which):
            load.wait()

    @pl.when(live)
    def _():
        node = lax.broadcasted_iota(jnp.int32, (BLK, BLK), 0) + block * BLK

        def finish(with_sink):
            worst = zero
            for head in (0, 1):
                for pair in range(groups // 2):
                    parts = []
                    for g in (2 * pair, 2 * pair + 1):
                        rows = slice(g * BLK, (g + 1) * BLK)
                        under = sums[head, rows, BLK : 2 * BLK]
                        if with_sink:
                            under = under + sink_ref[1, sink_base + head * groups + g]
                        worst = jnp.maximum(worst, under)
                        parts.append(sums[head, rows, 0:BLK] / under)
                    if head == 0:
                        joined = jnp.where(low, parts[0], pltpu.roll(parts[1], HD, 1))
                    else:
                        joined = jnp.where(low, pltpu.roll(parts[0], HD, 1), parts[1])
                    cols = slice((head * groups // 2 + pair) * BLK, (head * groups // 2 + pair + 1) * BLK)
                    out_ref[:, cols] = jnp.where(node < node_total, joined, zero).astype(jnp.bfloat16)
            return worst

        def quick(head, carry):
            weights = jnp.exp(contract_last(qx[head], kx[...])).astype(jnp.bfloat16)
            sums[head] = dot(weights, vx[...])
            return carry

        lax.fori_loop(0, 2, quick, 0)
        worst = finish(True)

        @pl.when(jnp.logical_not(jnp.max(worst) < TRUSTED))
        def _():
            def careful(g, carry):
                for head in (0, 1):
                    rows = pl.ds(pl.multiple_of(g * BLK, BLK), BLK)
                    scores = contract_last(qx[head, rows, :], kx[...])
                    sink = sink_ref[0, sink_base + head * groups + g]
                    peak = jnp.maximum(jnp.max(scores, axis=1, keepdims=True), sink)
                    weights = jnp.exp(scores - peak).astype(jnp.bfloat16)
                    part = dot(weights, vx[...])
                    sums[head, rows, 0:BLK] = part[:, 0:BLK]
                    sums[head, rows, BLK : 2 * BLK] = part[:, BLK : 2 * BLK] + jnp.exp(sink - peak)
                return carry

            lax.fori_loop(0, groups, careful, 0)
            finish(False)

    @pl.when(jnp.logical_not(live))
    def _():
        out_ref[...] = jnp.zeros_like(out_ref)


def attend(scal, here, there, sinks, for_busy, at, pairs, first, count, rows, tree_rows, before):
    q, *kv, bias = here
    q_got, *kv_got, bias_got = there
    cache_rows = kv[0].shape[0]
    width = q.shape[1] // (KVH // 2)
    keys = cache_rows + tree_rows
    per_core = KVH // 4
    anywhere = pl.BlockSpec(memory_space=pl.ANY)
    in_specs = [
        pl.BlockSpec((BLK, width), lambda p, i, s: (first + i, s[0] * per_core + at + p)),
        pl.BlockSpec((tree_rows, BLK), lambda p, i, s: (0, first + i)),
        pl.BlockSpec((BLK, width), lambda p, i, s: (first + i, at + p)),
        pl.BlockSpec((tree_rows, BLK), lambda p, i, s: (0, first + i)),
        *[anywhere] * 8,
        pl.BlockSpec(memory_space=pltpu.SMEM),
    ]
    operands = [q, bias, q_got, bias_got, *kv, *kv_got, sinks]
    aliases = {}
    if before is not None:
        aliases[1 + len(operands)] = 0
        in_specs.append(anywhere)
        operands.append(before)
    groups = width // HD // 2
    work = pairs * count * BLK * 2 * groups * keys
    return pl.pallas_call(
        functools.partial(attend_kernel, for_busy, len(aliases), first, at),
        grid_spec=pltpu.PrefetchScalarGridSpec(
            num_scalar_prefetch=1,
            grid=(pairs, count),
            in_specs=in_specs,
            out_specs=pl.BlockSpec((BLK, width), lambda p, i, s: (first + i, p)),
            scratch_shapes=[
                pltpu.VMEM((pairs, keys, 2 * BLK), jnp.bfloat16),
                pltpu.VMEM((pairs, keys, 2 * BLK), jnp.bfloat16),
                pltpu.VMEM((2, groups * BLK, 2 * BLK), jnp.bfloat16),
                pltpu.VMEM((2, groups * BLK, 2 * BLK), jnp.float32),
                pltpu.SemaphoreType.DMA((pairs, 4)),
            ],
        ),
        out_shape=jax.ShapeDtypeStruct((rows, pairs * width), jnp.bfloat16),
        input_output_aliases=aliases,
        compiler_params=pltpu.CompilerParams(vmem_limit_bytes=VMEM_LIMIT),
        cost_estimate=pl.CostEstimate(
            flops=work * 2 * 4 * BLK, bytes_accessed=8 * keys * BLK, transcendentals=work
        ),
        name="attend",
    )(scal, *operands)


def tree_bias(words_t, key_total):
    spread = jnp.repeat(words_t, 32, axis=0)
    shift = (jnp.arange(key_total, dtype=jnp.int32) % 32)[:, None]
    flag = jnp.bitwise_and(lax.shift_right_logical(spread, jnp.broadcast_to(shift, spread.shape)), 1)
    return jnp.where(flag > 0, 0.0, MASKED).astype(jnp.bfloat16)


TILES = 6


def project_kernel(blocks, info, *refs):
    busy_mine, busy_got, light_mine, light_got = refs[0:2], refs[2:4], refs[4], refs[5]
    weights = refs[6 : 6 + blocks]
    own_ref, other_ref, attended, x, w, blank, came, left = refs[6 + blocks :]
    step = pl.program_id(0)
    nodes, width = busy_mine[0].shape
    few = light_mine.shape[0]
    depth = weights[0].shape[1]
    here_busy = info[0] > 0

    def loads(core, mine):
        busy, light = (busy_mine, light_mine) if mine else (busy_got, light_got)
        base = core * 2 * width
        for m in (0, 1):
            yield pltpu.make_async_copy(
                busy[m], x.at[pl.ds(0, nodes), pl.ds(base + m * width, width)], came.at[core, m]
            )
        yield pltpu.make_async_copy(light, x.at[pl.ds(nodes, few), pl.ds(base, 2 * width)], came.at[core, 2])

    def busy_stores():
        return [pltpu.make_async_copy(x.at[pl.ds(0, nodes), :], attended, left.at[0])]

    def light_stores():
        return [
            pltpu.make_async_copy(x.at[pl.ds(nodes, few), :], attended.at[pl.ds(0, few), :], left.at[0]),
            pltpu.make_async_copy(blank, attended.at[pl.ds(few, nodes - few), :], left.at[1]),
        ]

    def for_either(act):
        @pl.when(here_busy)
        def _():
            for copy in busy_stores():
                act(copy)

        @pl.when(jnp.logical_not(here_busy))
        def _():
            for copy in light_stores():
                act(copy)

    @pl.when(step == 0)
    def _():
        for core in (0, 1):
            for mine in (True, False):

                @pl.when((info[1] == core) == mine)
                def _():
                    for copy in loads(core, mine):
                        copy.start()

        blank[...] = jnp.zeros_like(blank)

    for k in range(blocks):
        w[:, pl.ds(pl.multiple_of(info[2 + k] * depth, depth), depth)] = weights[k][...]

    @pl.when(step == 0)
    def _():
        for core in (0, 1):
            for copy in loads(core, True):
                copy.wait()
        for_either(lambda copy: copy.start())

    done = contract_last(w[...], x[...]).astype(jnp.bfloat16)
    rest = jnp.zeros((done.shape[0], nodes - few), jnp.bfloat16)

    @pl.when(here_busy)
    def _():
        own_ref[...] = done[:, :nodes]
        other_ref[:, 0:few] = done[:, nodes:]
        other_ref[:, few:] = rest

    @pl.when(jnp.logical_not(here_busy))
    def _():
        other_ref[...] = done[:, :nodes]
        own_ref[:, 0:few] = done[:, nodes:]
        own_ref[:, few:] = rest

    @pl.when(step == pl.num_programs(0) - 1)
    def _():
        for_either(lambda copy: copy.wait())


def project(info, pieces, blocks):
    columns, depth = blocks[0].shape
    tile = columns // TILES
    nodes, few = pieces[0].shape[0], pieces[4].shape[0]
    total = depth * len(blocks)
    anywhere = pl.BlockSpec(memory_space=pl.ANY)
    return pl.pallas_call(
        functools.partial(project_kernel, len(blocks)),
        grid_spec=pltpu.PrefetchScalarGridSpec(
            num_scalar_prefetch=1,
            grid=(TILES,),
            in_specs=[anywhere] * len(pieces)
            + [pl.BlockSpec((tile, depth), lambda i, s: (i, 0))] * len(blocks),
            out_specs=[
                pl.BlockSpec((tile, nodes), lambda i, s: (s[1] * TILES + i, 0)),
                pl.BlockSpec((tile, nodes), lambda i, s: (i, 0)),
                anywhere,
            ],
            scratch_shapes=[
                pltpu.VMEM((nodes + few, total), jnp.bfloat16),
                pltpu.VMEM((tile, total), jnp.bfloat16),
                pltpu.VMEM((nodes - few, total), jnp.bfloat16),
                pltpu.SemaphoreType.DMA((2, 3)),
                pltpu.SemaphoreType.DMA((2,)),
            ],
        ),
        out_shape=[
            jax.ShapeDtypeStruct((2 * columns, nodes), jnp.bfloat16),
            jax.ShapeDtypeStruct((columns, nodes), jnp.bfloat16),
            jax.ShapeDtypeStruct((nodes, total), jnp.bfloat16),
        ],
        compiler_params=pltpu.CompilerParams(vmem_limit_bytes=VMEM_LIMIT),
        cost_estimate=pl.CostEstimate(
            flops=2 * (nodes + few) * columns * total, bytes_accessed=2 * columns * total, transcendentals=0
        ),
        name="project",
    )(info, *pieces, *blocks)


def on_device(plane, line, args):
    (
        q_nodes, k_cache, v_cache, k_tree, v_tree, anc_bits, node_count, cache_len, sinks, o_weight,
    ) = args
    gx = lax.axis_index("gx")
    gy = lax.axis_index("gy")
    core = gy % 2
    far = 1 - core
    z = gy // 2
    is_busy = (gx + gy) % 2 == 0
    places = [(a, b, c) for a in range(plane) for b in range(line) for c in range(2)]

    def number(a, b, c):
        return (a * line + b) * 2 + c

    def moved(x, to):
        pairs = [(number(*p), number(*to(*p))) for p in places]
        return lax.ppermute(x, AXES, pairs)

    def swapped(x):
        return moved(x, lambda a, b, c: (a, b, 1 - c))

    q, kc, vc, kt, vt = q_nodes[0], k_cache[0], v_cache[0], k_tree[0], v_tree[0]
    node_total = q.shape[0]
    tree_rows = kt.shape[0]
    columns = o_weight.shape[1] // 2
    half_q = q.shape[1] // 2

    w_t = o_weight.T
    w_mine = lax.dynamic_slice_in_dim(w_t, core * columns, columns, 0)
    w_theirs = swapped(lax.dynamic_slice_in_dim(w_t, far * columns, columns, 0))
    b0 = jnp.where(
        core == 0,
        jnp.concatenate([w_mine, w_theirs], axis=1),
        jnp.concatenate([w_theirs, w_mine], axis=1),
    )

    words_t = anc_bits[0].T
    words = words_t.shape[0]
    spot = jnp.arange(words + 2, dtype=jnp.int32)[:, None]
    note = jnp.pad(words_t, ((0, 2), (0, 0)))
    note = jnp.where(spot == words, node_count[0], jnp.where(spot == words + 1, cache_len[0], note))
    kv = (kc, vc, kt, vt)
    kv_got = tuple(swapped(a) for a in kv)
    q_got = swapped(lax.dynamic_slice_in_dim(q, far * half_q, half_q, 1))
    note_got = swapped(note)
    here = (q, *kv, tree_bias(words_t, tree_rows))
    there = (q_got, *kv_got, tree_bias(note_got[:words], tree_rows))

    def table(values):
        spot = jnp.arange(len(values), dtype=jnp.int32)
        out = jnp.zeros((len(values),), jnp.int32)
        for i, v in enumerate(values):
            out = jnp.where(spot == i, v, out)
        return out

    flags = table(
        [core, node_count[0], cache_len[0], is_busy.astype(jnp.int32), note_got[words, 0], note_got[words + 1, 0]]
    )
    sink_table = jnp.stack([sinks, jnp.exp(sinks)])
    half = node_total // BLK // 2

    def attend_busy(at, first, before):
        return attend(
            flags, here, there, sink_table, True, at, 1, first, half, node_total, tree_rows, before
        )

    def attend_light():
        return attend(flags, here, there, sink_table, False, 0, KVH // 4, 0, 1, BLK, BLK, None)

    direct = plane == 4 and line == 4

    def along_x(x):
        return moved(x, lambda a, b, c: (a ^ 1, b, c))

    def along_y(x):
        return moved(x, lambda a, b, c: (a ^ 2, b, c))

    def along_z(x, by):
        return moved(x, lambda a, b, c: (a, (b + by) % line, c))

    def together(*arrays):
        return lax.optimization_barrier(arrays) if direct else arrays

    if direct:
        x0, y0, z1 = along_x(b0), along_y(b0), along_z(b0, 1)
    else:
        x0 = y0 = z1 = b0
    busy0 = attend_busy(0, 0, None)
    busy0, b0, x0, y0, z1 = together(busy0, b0, x0, y0, z1)
    if direct:
        d0, y1, z3, x1 = along_x(y0), along_y(z1), along_z(b0, 3), along_x(z1)
    else:
        d0 = y1 = z3 = x1 = b0
    busy0 = attend_busy(0, half, busy0)
    busy0, d0, y1, z3, z1 = together(busy0, d0, y1, z3, z1)
    if direct:
        z2, y3 = along_z(z1, 1), along_y(z3)
    else:
        z2 = y3 = b0
    busy1 = attend_busy(1, 0, None)
    busy1, x1, z2, z3, d0 = together(busy1, x1, z2, z3, d0)
    if direct:
        x2, y2, x3 = along_x(z2), along_y(z2), along_x(z3)
        d1, d3 = along_z(d0, 1), along_z(d0, 3)
    else:
        x2 = y2 = x3 = d1 = d3 = b0
    busy1 = attend_busy(1, half, busy1)
    busy1, x2 = together(busy1, x2)
    d2 = along_y(x2) if direct else b0
    light = attend_light()
    got0, got1, light_got = swapped(busy0), swapped(busy1), swapped(light)

    if direct:
        slots = {}
        info = [is_busy.astype(jnp.int32), core]
        for dz in (0, 1, 3, 2):
            for flip in (0, 1, 2, 3):
                slots[(dz, flip)] = len(info)
                info.append((gx ^ flip) * line + (z - dz) % line)
        info = table(info)
        blocks = [
            (b0, (0, 0)), (x0, (0, 1)), (y0, (0, 2)), (d0, (0, 3)),
            (z1, (1, 0)), (x1, (1, 1)), (y1, (1, 2)), (d1, (1, 3)),
            (z3, (3, 0)), (x3, (3, 1)), (y3, (3, 2)), (d3, (3, 3)),
            (z2, (2, 0)), (x2, (2, 1)), (y2, (2, 2)), (d2, (2, 3)),
        ]
        order = sorted(blocks, key=lambda b: slots[b[1]])
        full, other_half, attended = project(info, (busy0, busy1, got0, got1, light, light_got), [b for b, _ in order])
        full = lax.dynamic_update_slice(full, swapped(other_half), (far * columns, 0))
        projected = full.T
    else:

        def in_order(mine, got):
            return jnp.where(
                core == 0, jnp.concatenate([*mine, *got], axis=1), jnp.concatenate([*got, *mine], axis=1)
            )

        padded = jnp.pad(in_order([light], [light_got]), ((0, node_total - BLK), (0, 0)))
        attended = jnp.where(is_busy, in_order([busy0, busy1], [got0, got1]), padded)
        w_all = lax.all_gather(o_weight, AXES, axis=0, tiled=True)
        projected = dot(attended, w_all).astype(jnp.bfloat16)
    return attended[None], projected[None]


def solution(mesh):
    plane, line = mesh.shape["gx"], mesh.shape["gy"] // 2
    rows = P(AXES, None, None)
    placed = (rows, rows, rows, rows, rows, rows, P(AXES), P(AXES), P(), P(AXES, None))

    def run(*args):
        return on_device(plane, line, args)

    return jax.shard_map(run, mesh=mesh, in_specs=placed, out_specs=(rows, rows), check_vma=False)
```

```python
import functools

import jax
import jax.numpy as jnp
from jax import lax
from jax.experimental import pallas as pl
from jax.experimental.pallas import tpu as pltpu
from jax.sharding import PartitionSpec as P

KVH = 8
HD = 64
BLK = 128
MASKED = -1e30
TRUSTED = 1e26
AXES = ("gx", "gy")
VMEM_LIMIT = 60 * 1024 * 1024


def contract_last(a, b):
    return lax.dot_general(a, b, (((1,), (1,)), ((), ())), preferred_element_type=jnp.float32)


def dot(a, b):
    return jnp.dot(a, b, preferred_element_type=jnp.float32)


def attend_kernel(for_busy, chained, first, at, scal, *refs):
    q_here, bias_here, q_there, bias_there = refs[0:4]
    here, there = refs[4:8], refs[8:12]
    sink_ref = refs[12]
    out_ref, kx_all, vx_all, qx, sums, arrived = refs[13 + chained :]
    step = pl.program_id(1)
    block = step + first
    here_busy = scal[3] > 0
    use_here = here_busy if for_busy else jnp.logical_not(here_busy)
    cache_rows = here[0].shape[0]
    key_rows = kx_all.shape[1]
    tree_rows = key_rows - cache_rows
    groups = q_here.shape[1] // HD // 2
    node_total = jnp.where(use_here, scal[1], scal[4])
    cache_total = jnp.where(use_here, scal[2], scal[5])
    which = pl.program_id(0)
    pairs = kx_all.shape[0]
    kx, vx = kx_all.at[which], vx_all.at[which]
    lane_pair = scal[0] * (KVH // 4) + at + which
    sink_base = lane_pair * (2 * groups)

    def loads(source, pair):
        cols = pl.ds(pl.multiple_of((scal[0] * (KVH // 4) + at + pair) * BLK, BLK), BLK)
        kc_ref, vc_ref, kt_ref, vt_ref = source
        low, high = pl.ds(0, cache_rows), pl.ds(cache_rows, tree_rows)
        lanes, tree = pl.ds(0, BLK), pl.ds(0, tree_rows)
        return (
            pltpu.make_async_copy(kc_ref.at[low, cols], kx_all.at[pair, low, lanes], arrived.at[pair, 0]),
            pltpu.make_async_copy(kt_ref.at[tree, cols], kx_all.at[pair, high, lanes], arrived.at[pair, 1]),
            pltpu.make_async_copy(vc_ref.at[low, cols], vx_all.at[pair, low, lanes], arrived.at[pair, 2]),
            pltpu.make_async_copy(vt_ref.at[tree, cols], vx_all.at[pair, high, lanes], arrived.at[pair, 3]),
        )

    @pl.when((step == 0) & (which == 0))
    def _():
        @pl.when(use_here)
        def _():
            for pair in range(pairs):
                for load in loads(here, pair):
                    load.start()

        @pl.when(jnp.logical_not(use_here))
        def _():
            for pair in range(pairs):
                for load in loads(there, pair):
                    load.start()

        row = lax.broadcasted_iota(jnp.int32, (cache_rows, BLK), 0)
        hidden = jnp.where(row < cache_total, 0.0, MASKED).astype(jnp.bfloat16)
        for pair in range(pairs):
            vx_all[pair, :, BLK : 2 * BLK] = jnp.ones((key_rows, BLK), jnp.bfloat16)
            kx_all[pair, 0:cache_rows, BLK : 2 * BLK] = hidden
        src = lax.broadcasted_iota(jnp.int32, (BLK, BLK), 0)
        dst = lax.broadcasted_iota(jnp.int32, (BLK, BLK), 1)
        own = jnp.where(src == dst, 1.0, 0.0).astype(jnp.bfloat16)
        for head in (0, 1):
            for g in range(groups):
                qx[head, g * BLK : (g + 1) * BLK, BLK : 2 * BLK] = own

    live = block * BLK < node_total
    lane = lax.broadcasted_iota(jnp.int32, (BLK, BLK), 1)
    low = lane < HD
    zero = jnp.zeros((BLK, BLK), jnp.float32)

    @pl.when(live)
    def _():
        kx[cache_rows:key_rows, BLK : 2 * BLK] = jnp.where(use_here, bias_here[...], bias_there[...])
        for head in (0, 1):
            for pair in range(groups // 2):
                cols = slice((head * groups // 2 + pair) * BLK, (head * groups // 2 + pair + 1) * BLK)
                both = jnp.where(use_here, q_here[:, cols], q_there[:, cols]).astype(jnp.float32) * (HD**-0.5)
                turned = pltpu.roll(both, HD, 1)
                if head == 0:
                    upper, lower = jnp.where(low, both, zero), jnp.where(low, turned, zero)
                else:
                    upper, lower = jnp.where(low, zero, turned), jnp.where(low, zero, both)
                at_row = 2 * pair * BLK
                qx[head, at_row : at_row + BLK, 0:BLK] = upper.astype(jnp.bfloat16)
                qx[head, at_row + BLK : at_row + 2 * BLK, 0:BLK] = lower.astype(jnp.bfloat16)

    @pl.when(step == 0)
    def _():
        for load in loads(here, which):
            load.wait()

    @pl.when(live)
    def _():
        node = lax.broadcasted_iota(jnp.int32, (BLK, BLK), 0) + block * BLK

        def finish(with_sink):
            worst = zero
            for head in (0, 1):
                for pair in range(groups // 2):
                    parts = []
                    for g in (2 * pair, 2 * pair + 1):
                        rows = slice(g * BLK, (g + 1) * BLK)
                        under = sums[head, rows, BLK : 2 * BLK]
                        if with_sink:
                            under = under + sink_ref[1, sink_base + head * groups + g]
                        worst = jnp.maximum(worst, under)
                        parts.append(sums[head, rows, 0:BLK] / under)
                    if head == 0:
                        joined = jnp.where(low, parts[0], pltpu.roll(parts[1], HD, 1))
                    else:
                        joined = jnp.where(low, pltpu.roll(parts[0], HD, 1), parts[1])
                    cols = slice((head * groups // 2 + pair) * BLK, (head * groups // 2 + pair + 1) * BLK)
                    out_ref[:, cols] = jnp.where(node < node_total, joined, zero).astype(jnp.bfloat16)
            return worst

        def quick(head, carry):
            weights = jnp.exp(contract_last(qx[head], kx[...])).astype(jnp.bfloat16)
            sums[head] = dot(weights, vx[...])
            return carry

        lax.fori_loop(0, 2, quick, 0)
        worst = finish(True)

        @pl.when(jnp.logical_not(jnp.max(worst) < TRUSTED))
        def _():
            def careful(g, carry):
                for head in (0, 1):
                    rows = pl.ds(pl.multiple_of(g * BLK, BLK), BLK)
                    scores = contract_last(qx[head, rows, :], kx[...])
                    sink = sink_ref[0, sink_base + head * groups + g]
                    peak = jnp.maximum(jnp.max(scores, axis=1, keepdims=True), sink)
                    weights = jnp.exp(scores - peak).astype(jnp.bfloat16)
                    part = dot(weights, vx[...])
                    sums[head, rows, 0:BLK] = part[:, 0:BLK]
                    sums[head, rows, BLK : 2 * BLK] = part[:, BLK : 2 * BLK] + jnp.exp(sink - peak)
                return carry

            lax.fori_loop(0, groups, careful, 0)
            finish(False)

    @pl.when(jnp.logical_not(live))
    def _():
        out_ref[...] = jnp.zeros_like(out_ref)


def attend(scal, here, there, sinks, for_busy, at, pairs, first, count, rows, tree_rows, before):
    q, *kv, bias = here
    q_got, *kv_got, bias_got = there
    cache_rows = kv[0].shape[0]
    width = q.shape[1] // (KVH // 2)
    keys = cache_rows + tree_rows
    per_core = KVH // 4
    anywhere = pl.BlockSpec(memory_space=pl.ANY)
    in_specs = [
        pl.BlockSpec((BLK, width), lambda p, i, s: (first + i, s[0] * per_core + at + p)),
        pl.BlockSpec((tree_rows, BLK), lambda p, i, s: (0, first + i)),
        pl.BlockSpec((BLK, width), lambda p, i, s: (first + i, at + p)),
        pl.BlockSpec((tree_rows, BLK), lambda p, i, s: (0, first + i)),
        *[anywhere] * 8,
        pl.BlockSpec(memory_space=pltpu.SMEM),
    ]
    operands = [q, bias, q_got, bias_got, *kv, *kv_got, sinks]
    aliases = {}
    if before is not None:
        aliases[1 + len(operands)] = 0
        in_specs.append(anywhere)
        operands.append(before)
    groups = width // HD // 2
    work = pairs * count * BLK * 2 * groups * keys
    return pl.pallas_call(
        functools.partial(attend_kernel, for_busy, len(aliases), first, at),
        grid_spec=pltpu.PrefetchScalarGridSpec(
            num_scalar_prefetch=1,
            grid=(pairs, count),
            in_specs=in_specs,
            out_specs=pl.BlockSpec((BLK, width), lambda p, i, s: (first + i, p)),
            scratch_shapes=[
                pltpu.VMEM((pairs, keys, 2 * BLK), jnp.bfloat16),
                pltpu.VMEM((pairs, keys, 2 * BLK), jnp.bfloat16),
                pltpu.VMEM((2, groups * BLK, 2 * BLK), jnp.bfloat16),
                pltpu.VMEM((2, groups * BLK, 2 * BLK), jnp.float32),
                pltpu.SemaphoreType.DMA((pairs, 4)),
            ],
        ),
        out_shape=jax.ShapeDtypeStruct((rows, pairs * width), jnp.bfloat16),
        input_output_aliases=aliases,
        compiler_params=pltpu.CompilerParams(vmem_limit_bytes=VMEM_LIMIT),
        cost_estimate=pl.CostEstimate(
            flops=work * 2 * 4 * BLK, bytes_accessed=8 * keys * BLK, transcendentals=work
        ),
        name="attend",
    )(scal, *operands)


def tree_bias(words_t, key_total):
    spread = jnp.repeat(words_t, 32, axis=0)
    shift = (jnp.arange(key_total, dtype=jnp.int32) % 32)[:, None]
    flag = jnp.bitwise_and(lax.shift_right_logical(spread, jnp.broadcast_to(shift, spread.shape)), 1)
    return jnp.where(flag > 0, 0.0, MASKED).astype(jnp.bfloat16)


TILES = 6


def project_kernel(blocks, info, *refs):
    busy_mine, busy_got, light_mine, light_got = refs[0:2], refs[2:4], refs[4], refs[5]
    weights = refs[6 : 6 + blocks]
    own_ref, other_ref, attended, x, blank, came, left = refs[6 + blocks :]
    step = pl.program_id(0)
    nodes, width = busy_mine[0].shape
    few = light_mine.shape[0]
    depth = weights[0].shape[1]
    here_busy = info[0] > 0

    def loads(core, mine):
        busy, light = (busy_mine, light_mine) if mine else (busy_got, light_got)
        base = core * 2 * width
        for m in (0, 1):
            yield pltpu.make_async_copy(
                busy[m], x.at[pl.ds(0, nodes), pl.ds(base + m * width, width)], came.at[core, m]
            )
        yield pltpu.make_async_copy(light, x.at[pl.ds(nodes, few), pl.ds(base, 2 * width)], came.at[core, 2])

    def busy_stores():
        return [pltpu.make_async_copy(x.at[pl.ds(0, nodes), :], attended, left.at[0])]

    def light_stores():
        return [
            pltpu.make_async_copy(x.at[pl.ds(nodes, few), :], attended.at[pl.ds(0, few), :], left.at[0]),
            pltpu.make_async_copy(blank, attended.at[pl.ds(few, nodes - few), :], left.at[1]),
        ]

    def for_either(act):
        @pl.when(here_busy)
        def _():
            for copy in busy_stores():
                act(copy)

        @pl.when(jnp.logical_not(here_busy))
        def _():
            for copy in light_stores():
                act(copy)

    @pl.when(step == 0)
    def _():
        for core in (0, 1):
            for mine in (True, False):

                @pl.when((info[1] == core) == mine)
                def _():
                    for copy in loads(core, mine):
                        copy.start()

        blank[...] = jnp.zeros_like(blank)

    @pl.when(step == 0)
    def _():
        for core in (0, 1):
            for copy in loads(core, True):
                copy.wait()
        for_either(lambda copy: copy.start())

    part = None
    for k in range(blocks):
        term = contract_last(weights[k][...], x[:, pl.ds(pl.multiple_of(info[2 + k] * depth, depth), depth)])
        part = term if part is None else part + term
    done = part.astype(jnp.bfloat16)
    rest = jnp.zeros((done.shape[0], nodes - few), jnp.bfloat16)

    @pl.when(here_busy)
    def _():
        own_ref[...] = done[:, :nodes]
        other_ref[:, 0:few] = done[:, nodes:]
        other_ref[:, few:] = rest

    @pl.when(jnp.logical_not(here_busy))
    def _():
        other_ref[...] = done[:, :nodes]
        own_ref[:, 0:few] = done[:, nodes:]
        own_ref[:, few:] = rest

    @pl.when(step == pl.num_programs(0) - 1)
    def _():
        for_either(lambda copy: copy.wait())


def project(info, pieces, blocks):
    columns, depth = blocks[0].shape
    tile = columns // TILES
    nodes, few = pieces[0].shape[0], pieces[4].shape[0]
    total = depth * len(blocks)
    anywhere = pl.BlockSpec(memory_space=pl.ANY)
    return pl.pallas_call(
        functools.partial(project_kernel, len(blocks)),
        grid_spec=pltpu.PrefetchScalarGridSpec(
            num_scalar_prefetch=1,
            grid=(TILES,),
            in_specs=[anywhere] * len(pieces)
            + [pl.BlockSpec((tile, depth), lambda i, s: (i, 0))] * len(blocks),
            out_specs=[
                pl.BlockSpec((tile, nodes), lambda i, s: (s[1] * TILES + i, 0)),
                pl.BlockSpec((tile, nodes), lambda i, s: (i, 0)),
                anywhere,
            ],
            scratch_shapes=[
                pltpu.VMEM((nodes + few, total), jnp.bfloat16),
                pltpu.VMEM((nodes - few, total), jnp.bfloat16),
                pltpu.SemaphoreType.DMA((2, 3)),
                pltpu.SemaphoreType.DMA((2,)),
            ],
        ),
        out_shape=[
            jax.ShapeDtypeStruct((2 * columns, nodes), jnp.bfloat16),
            jax.ShapeDtypeStruct((columns, nodes), jnp.bfloat16),
            jax.ShapeDtypeStruct((nodes, total), jnp.bfloat16),
        ],
        compiler_params=pltpu.CompilerParams(vmem_limit_bytes=VMEM_LIMIT),
        cost_estimate=pl.CostEstimate(
            flops=2 * (nodes + few) * columns * total, bytes_accessed=2 * columns * total, transcendentals=0
        ),
        name="project",
    )(info, *pieces, *blocks)


def on_device(plane, line, args):
    (
        q_nodes, k_cache, v_cache, k_tree, v_tree, anc_bits, node_count, cache_len, sinks, o_weight,
    ) = args
    gx = lax.axis_index("gx")
    gy = lax.axis_index("gy")
    core = gy % 2
    far = 1 - core
    z = gy // 2
    is_busy = (gx + gy) % 2 == 0
    places = [(a, b, c) for a in range(plane) for b in range(line) for c in range(2)]

    def number(a, b, c):
        return (a * line + b) * 2 + c

    def moved(x, to):
        pairs = [(number(*p), number(*to(*p))) for p in places]
        return lax.ppermute(x, AXES, pairs)

    def swapped(x):
        return moved(x, lambda a, b, c: (a, b, 1 - c))

    q, kc, vc, kt, vt = q_nodes[0], k_cache[0], v_cache[0], k_tree[0], v_tree[0]
    node_total = q.shape[0]
    tree_rows = kt.shape[0]
    columns = o_weight.shape[1] // 2
    half_q = q.shape[1] // 2

    w_t = o_weight.T
    w_mine = lax.dynamic_slice_in_dim(w_t, core * columns, columns, 0)
    w_theirs = swapped(lax.dynamic_slice_in_dim(w_t, far * columns, columns, 0))
    b0 = jnp.where(
        core == 0,
        jnp.concatenate([w_mine, w_theirs], axis=1),
        jnp.concatenate([w_theirs, w_mine], axis=1),
    )

    words_t = anc_bits[0].T
    words = words_t.shape[0]
    spot = jnp.arange(words + 2, dtype=jnp.int32)[:, None]
    note = jnp.pad(words_t, ((0, 2), (0, 0)))
    note = jnp.where(spot == words, node_count[0], jnp.where(spot == words + 1, cache_len[0], note))
    kv = (kc, vc, kt, vt)
    kv_got = tuple(swapped(a) for a in kv)
    later_q, _ = lax.optimization_barrier((q, b0)) if plane == 4 and line == 4 else (q, b0)
    q_got = swapped(lax.dynamic_slice_in_dim(later_q, far * half_q, half_q, 1))
    note_got = swapped(note)
    here = (q, *kv, tree_bias(words_t, tree_rows))
    there = (q_got, *kv_got, tree_bias(note_got[:words], tree_rows))

    def table(values):
        spot = jnp.arange(len(values), dtype=jnp.int32)
        out = jnp.zeros((len(values),), jnp.int32)
        for i, v in enumerate(values):
            out = jnp.where(spot == i, v, out)
        return out

    flags = table(
        [core, node_count[0], cache_len[0], is_busy.astype(jnp.int32), note_got[words, 0], note_got[words + 1, 0]]
    )
    sink_table = jnp.stack([sinks, jnp.exp(sinks)])
    half = node_total // BLK // 2

    def attend_busy(at, first, before):
        reach = (first + half) * BLK
        return attend(flags, here, there, sink_table, True, at, 1, first, half, node_total, reach, before)

    def attend_light():
        return attend(flags, here, there, sink_table, False, 0, KVH // 4, 0, 1, BLK, BLK, None)

    direct = plane == 4 and line == 4

    def along_x(x):
        return moved(x, lambda a, b, c: (a ^ 1, b, c))

    def along_y(x):
        return moved(x, lambda a, b, c: (a ^ 2, b, c))

    def along_z(x, by):
        return moved(x, lambda a, b, c: (a, (b + by) % line, c))

    def together(*arrays):
        return lax.optimization_barrier(arrays) if direct else arrays

    if direct:
        x0, y0, z1 = along_x(b0), along_y(b0), along_z(b0, 1)
    else:
        x0 = y0 = z1 = b0
    busy0 = attend_busy(0, 0, None)
    busy0, b0, x0, y0, z1 = together(busy0, b0, x0, y0, z1)
    if direct:
        d0, y1, z3, x1 = along_x(y0), along_y(z1), along_z(b0, 3), along_x(z1)
    else:
        d0 = y1 = z3 = x1 = b0
    busy0 = attend_busy(0, half, busy0)
    busy0, d0, y1, z3, z1 = together(busy0, d0, y1, z3, z1)
    if direct:
        z2, y3 = along_z(z1, 1), along_y(z3)
    else:
        z2 = y3 = b0
    busy1 = attend_busy(1, 0, None)
    busy1, x1, z2, z3, d0 = together(busy1, x1, z2, z3, d0)
    if direct:
        x2, y2, x3 = along_x(z2), along_y(z2), along_x(z3)
        d1, d3 = along_z(d0, 1), along_z(d0, 3)
    else:
        x2 = y2 = x3 = d1 = d3 = b0
    busy1 = attend_busy(1, half, busy1)
    busy1, x2 = together(busy1, x2)
    d2 = along_y(x2) if direct else b0
    light = attend_light()
    got0, got1, light_got = swapped(busy0), swapped(busy1), swapped(light)

    if direct:
        slots = {}
        info = [is_busy.astype(jnp.int32), core]
        for dz in (0, 1, 3, 2):
            for flip in (0, 1, 2, 3):
                slots[(dz, flip)] = len(info)
                info.append((gx ^ flip) * line + (z - dz) % line)
        info = table(info)
        blocks = [
            (b0, (0, 0)), (x0, (0, 1)), (y0, (0, 2)), (d0, (0, 3)),
            (z1, (1, 0)), (x1, (1, 1)), (y1, (1, 2)), (d1, (1, 3)),
            (z3, (3, 0)), (x3, (3, 1)), (y3, (3, 2)), (d3, (3, 3)),
            (z2, (2, 0)), (x2, (2, 1)), (y2, (2, 2)), (d2, (2, 3)),
        ]
        order = sorted(blocks, key=lambda b: slots[b[1]])
        full, other_half, attended = project(info, (busy0, busy1, got0, got1, light, light_got), [b for b, _ in order])
        full = lax.dynamic_update_slice(full, swapped(other_half), (far * columns, 0))
        projected = full.T
    else:

        def in_order(mine, got):
            return jnp.where(
                core == 0, jnp.concatenate([*mine, *got], axis=1), jnp.concatenate([*got, *mine], axis=1)
            )

        padded = jnp.pad(in_order([light], [light_got]), ((0, node_total - BLK), (0, 0)))
        attended = jnp.where(is_busy, in_order([busy0, busy1], [got0, got1]), padded)
        w_all = lax.all_gather(o_weight, AXES, axis=0, tiled=True)
        projected = dot(attended, w_all).astype(jnp.bfloat16)
    return attended[None], projected[None]


def solution(mesh):
    plane, line = mesh.shape["gx"], mesh.shape["gy"] // 2
    rows = P(AXES, None, None)
    placed = (rows, rows, rows, rows, rows, rows, P(AXES), P(AXES), P(), P(AXES, None))

    def run(*args):
        return on_device(plane, line, args)

    return jax.shard_map(run, mesh=mesh, in_specs=placed, out_specs=(rows, rows), check_vma=False)
```
